32 devices in a mesh: groups: 2 (over y), blk: 4 (over z), tile: 2 (over x), sub: 2 (over core).
Axes of the slice: x: 2, y: 2, z: 4, core: 2. Of those that a mesh axis runs over, the one named last changes fastest.
Arguments:
- raw_desc: bfloat16 [4096, 1536], P(('groups', 'blk', 'tile')), parts along dimension 0, may hold values from -11 to 11
- desc_mean: float32 [1536], replicated, may hold values from -6 to 6
- whitening: bfloat16 [1536, 256], P(None, 'sub'), may hold values from -0.15625 to 0.15625
Outputs:
- augmented: float32 [4096, 256], P(('groups', 'blk', 'tile'), 'sub'), parts along dimension 0
The draws below stay inside these ranges and needn't reach their ends.
There are 2 independent parts, one for each index of `groups`. The reference program is written for one: setup_inputs(seed, part) draws one part's arguments, and reference() takes and returns one part's arrays. A program takes and returns all parts, laid end to end along the dimension named above; an argument that names none is the same for every part. Nothing has to cross between parts.
All inputs are finite; a program needn't handle non-finite values.
Results may differ from the reference program's by a relative error of at most 0.0055.
The reference program's roundings to bfloat16 on the way count: a program that leaves them out, or rounds other values in their place, can miss the bound.
Values may be sent and summed in bfloat16 or wider, within the bound.
A program may use at most 128 MiB of HBM per device.

```python
import math
import jax
import jax.numpy as jnp
from jax import lax

RAW = 1536
WHITE = 256
IMAGES = 2048


def draw_raw_desc(key, part):
    first = jax.random.fold_in(jax.random.fold_in(key, 11), 0)
    values = jnp.clip(jax.random.normal(first, (IMAGES, RAW), jnp.float32), -6.0, 6.0)
    return values.astype(jnp.bfloat16)


def block_scale(key, shape, shards, low, high):
    level, own = 1.0, jax.random.fold_in(key, 6)
    for axis_at, parts in shards:
        heights = jnp.exp(jax.random.uniform(jax.random.fold_in(own, axis_at), (parts,), jnp.float32, low / len(shards), high / len(shards)))
        level = level * jnp.repeat(heights, shape[axis_at] // parts).reshape([-1 if axis == axis_at else 1 for axis in range(len(shape))])
    return level


def noise(key, shape, spread, reach, cuts=(), held_as=jnp.bfloat16):
    drawn = jax.random.normal(key, shape, jnp.float32) * spread
    if len(cuts) > 0:
        drawn = block_scale(key, shape, cuts, -0.22, 0.18) * drawn
    return jnp.clip(drawn, min=-reach, max=reach).astype(held_as)


def setup_inputs(seed: int = 0, part: int = 0) -> dict:
    key_list = jax.random.split(jax.random.key(seed), 4)
    part_splits = jax.random.split(jax.random.fold_in(key_list[3], part), 4)
    raw_desc = draw_raw_desc(jax.random.fold_in(jax.random.fold_in(key_list[3], part), 71), part)
    desc_mean = noise(key_list[1], (RAW,), 1.0, 6.0, (), jnp.float32)
    whitening = noise(key_list[2], (RAW, WHITE), RAW ** -0.5, 0.15625, ((1, 2),))
    return dict(raw_desc=raw_desc, desc_mean=desc_mean, whitening=whitening)


beta = 0.125

def reference(raw_desc, desc_mean, whitening):
    centred = (raw_desc.astype(jnp.float32) - desc_mean).astype(jnp.bfloat16)
    feats = jnp.dot(centred, whitening, preferred_element_type=jnp.float32).astype(jnp.bfloat16)
    feats_full = feats.astype(jnp.float32)
    images = feats.shape[0]
    block = math.gcd(images, 512)
    key_index = jnp.arange(images, dtype=jnp.int32)

    def one_block(which):
        start = (which * block).astype(jnp.int32)
        queries = lax.dynamic_slice_in_dim(feats_full, start, block, 0)
        scores = beta * jnp.dot(queries, feats_full.T, precision=lax.Precision.HIGHEST, preferred_element_type=jnp.float32)
        query_index = start + jnp.arange(block, dtype=jnp.int32)
        masked = query_index[:, None] == key_index[None, :]
        scores = jnp.where(masked, -jnp.inf, scores)
        top = lax.optimization_barrier(jnp.max(scores, axis=1))
        expo = jnp.where(masked, 0.0, jnp.exp(scores - top[:, None]))
        total = lax.optimization_barrier(jnp.sum(expo, axis=1))
        summed = jnp.dot(expo.astype(jnp.bfloat16), feats, preferred_element_type=jnp.float32)
        return summed / total[:, None]
    gathered = lax.map(one_block, jnp.arange(images // block, dtype=jnp.int32))
    gathered = gathered.reshape(images, feats.shape[1])
    mixed = feats_full + gathered
    return mixed * lax.rsqrt(lax.optimization_barrier(jnp.sum(mixed * mixed, axis=1, keepdims=True)) + 1e-06)
```

```python
import functools

import jax
import jax.numpy as jnp
from jax import lax
from jax.experimental import pallas as pl
from jax.experimental.pallas import tpu as pltpu
from jax.sharding import PartitionSpec as P

beta = 0.125
lowest = -1e30
slabs = 3
pieces = 2
MESH = pl.DeviceIdType.MESH


def repeat(start, stop, body):
    if stop - start <= 8:
        for k in range(start, stop):
            body(k)
    else:
        lax.fori_loop(start, stop, lambda k, _: (body(k), 0)[1], 0)


def other_than(me, k):
    return k + jnp.where(k >= me, 1, 0)


def kernel(
    blks, tiles,
    raw_hbm, mean_hbm, white_hbm, out_ref,
    raw, mean, white, keys, acc, stat,
    raw_sem, white_sem, mean_sem, sent, recv, pair_recv, ready_z, ready_x, gone, token,
):
    z, x, s = lax.axis_index("blk"), lax.axis_index("tile"), lax.axis_index("sub")
    other = 1 - s
    rows, width = keys.shape[1], keys.shape[2]
    chips = blks * tiles
    piece = rows // pieces
    slab = raw.shape[1] // slabs
    load_mean = pltpu.make_async_copy(mean_hbm, mean, mean_sem)
    load_mean.start()
    loads = []
    for c in range(slabs):
        at = pl.ds(c * slab, slab)
        loads.append((
            pltpu.make_async_copy(white_hbm.at[at], white.at[at], white_sem.at[c]),
            pltpu.make_async_copy(raw_hbm.at[:, at], raw.at[:, at], raw_sem.at[c]),
        ))
        for load in loads[-1]:
            load.start()

    barrier = pltpu.get_barrier_semaphore()

    def to_z(k):
        return {"blk": other_than(z, k)}

    def to_x(k):
        return {"tile": other_than(x, k)}

    def greet(device):
        pl.semaphore_signal(barrier, inc=1, device_id=device, device_id_type=MESH)

    greet({"sub": other})

    def greet_z(k):
        @pl.when(k >= z)
        def _():
            greet(to_z(k))

    def greet_x(k):
        @pl.when(k >= x)
        def _():
            greet(to_x(k))

    def answer_z(k):
        @pl.when(k < z)
        def _():
            pl.semaphore_signal(ready_z.at[z - 1], inc=1, device_id=to_z(k), device_id_type=MESH)

    def answer_x(k):
        @pl.when(k < x)
        def _():
            pl.semaphore_signal(ready_x.at[x - 1], inc=1, device_id=to_x(k), device_id_type=MESH)

    repeat(0, blks - 1, greet_z)
    repeat(0, tiles - 1, greet_x)
    pl.semaphore_wait(barrier, 1 + z + x)
    repeat(0, blks - 1, answer_z)
    repeat(0, tiles - 1, answer_x)

    def slot(zz, xx):
        return zz * tiles + xx

    mine = slot(z, x)

    def send(block, p, device, done=sent):
        at = keys.at[2 * block + s, pl.ds(p * piece, piece)]
        pltpu.make_async_remote_copy(
            at, at, done, recv.at[block, p], device_id=device, device_id_type=MESH,
        ).start()

    def left_home(k):
        pltpu.make_async_copy(keys.at[0], keys.at[0], gone.at[k]).wait()

    def share(block, p):
        at = keys.at[2 * block + s, pl.ds(p * piece, piece)]
        pltpu.make_async_remote_copy(
            at, at, sent, pair_recv.at[block], device_id={"sub": other}, device_id_type=MESH,
        ).start()

    load_mean.wait()
    half = None
    for c in range(slabs):
        at = pl.ds(c * slab, slab)
        for load in loads[c]:
            load.wait()
        centred = (raw[:, at].astype(jnp.float32) - mean[at].reshape(1, -1)).astype(jnp.bfloat16)
        term = jnp.dot(centred, white[at, :], preferred_element_type=jnp.float32)
        half = term if half is None else half + term
    keys[2 * mine + s] = half.astype(jnp.bfloat16)
    def push(k):
        for p in range(pieces):
            send(mine, p, to_z(k), gone.at[k])

    def rightward(k):
        @pl.when(k >= z)
        def _():
            pl.semaphore_wait(ready_z.at[k], 1)
            push(k)

    def leftward(k):
        @pl.when(k < z - 1)
        def _():
            push(k)

    def sideward(k):
        @pl.when(k >= x)
        def _():
            pl.semaphore_wait(ready_x.at[k], 1)
        for p in range(pieces):
            send(mine, p, to_x(k))

    for p in range(pieces):
        share(mine, p)

    @pl.when(z > 0)
    def _():
        push(0)

    @pl.when(z > 1)
    def _():
        push(z - 1)

    repeat(0, tiles - 1, sideward)
    repeat(0, blks - 1, rightward)

    @pl.when((z > 1) & (z + 1 < blks))
    def _():
        left_home(0)
        for r in range(2):
            pl.semaphore_signal(
                token, inc=1, device_id={"blk": z + 1, "sub": r}, device_id_type=MESH,
            )

    @pl.when(z > 2)
    def _():
        pl.semaphore_wait(token, 2)
    repeat(1, blks - 1, leftward)

    def take(block, forward):
        for p in range(pieces):
            at = keys.at[2 * block + s, pl.ds(p * piece, piece)]
            pltpu.make_async_copy(at, at, recv.at[block, p]).wait()
            if forward:
                repeat(0, tiles - 1, lambda k: send(block, p, to_x(k)))
            share(block, p)

    def both(block):
        return jnp.concatenate([keys[2 * block], keys[2 * block + 1]], axis=1)

    def paired(block):
        at = keys.at[2 * block + other]
        pltpu.make_async_copy(at, at, pair_recv.at[block]).wait()

    def scores_of(kk):
        nt = (((1,), (1,)), ((), ()))
        return beta * lax.dot_general(both(mine), kk, nt, preferred_element_type=jnp.float32)

    def attend(*blocks):
        for block in blocks:
            paired(block)
        kk = jnp.concatenate([both(block) for block in blocks], axis=0)
        sc = scores_of(kk)
        old = stat[0]
        top = jnp.maximum(old, jnp.max(sc, axis=1, keepdims=True))
        scale = jnp.exp(old - top)
        expo = jnp.exp(sc - top[:, :1])
        stat[0] = top
        stat[1] = stat[1] * scale + jnp.sum(expo, axis=1, keepdims=True)
        acc[...] = acc[...] * scale[:, :1] + jnp.dot(
            expo.astype(jnp.bfloat16), kk, preferred_element_type=jnp.float32
        )

    paired(mine)
    kk = both(mine)
    sc = scores_of(kk)
    query = lax.broadcasted_iota(jnp.int32, sc.shape, 0)
    key = lax.broadcasted_iota(jnp.int32, sc.shape, 1)
    masked = query == key
    sc = jnp.where(masked, lowest, sc)
    top = jnp.max(sc, axis=1, keepdims=True)
    expo = jnp.where(masked, 0.0, jnp.exp(sc - top))
    stat[0] = jnp.broadcast_to(top, stat.shape[1:])
    stat[1] = jnp.broadcast_to(jnp.sum(expo, axis=1, keepdims=True), stat.shape[1:])
    acc[...] = jnp.dot(expo.astype(jnp.bfloat16), kk, preferred_element_type=jnp.float32)

    def nth(k):
        return jnp.where(z == 0, blks - 1 - k, other_than(z, k))

    def z_block(k):
        return slot(nth(k), x)

    def x_block(k):
        return slot(z, other_than(x, k))

    def far_block(i):
        return slot(nth(i // (tiles - 1)), other_than(x, lax.rem(i, tiles - 1)))

    far = (blks - 1) * (tiles - 1)
    repeat(0, blks - 1, lambda k: take(z_block(k), True))
    repeat(0, tiles - 1, lambda k: take(x_block(k), False))
    if blks == 4 and tiles == 2:
        attend(z_block(0), z_block(1))
        take(far_block(0), False)
        attend(z_block(2), x_block(0))
        take(far_block(1), False)
        attend(far_block(0))
        take(far_block(2), False)
        attend(far_block(1))
        attend(far_block(2))
    else:
        repeat(0, blks - 1, lambda k: attend(z_block(k)))
        repeat(0, tiles - 1, lambda k: attend(x_block(k)))
        take(far_block(0), False)

        def across(i):
            take(far_block(i), False)
            attend(far_block(i - 1))

        repeat(1, far, across)
        attend(far_block(far - 1))

    whole = both(mine).astype(jnp.float32)
    mixed = whole + acc[...] * (1.0 / stat[1][:, :1])
    squares = jnp.sum(mixed * mixed, axis=1, keepdims=True)
    wanted = jnp.where(s == 0, mixed[:, :width], mixed[:, width:])
    out_ref[...] = wanted * lax.rsqrt(squares + 1e-06)

    def home(k):
        @pl.when((k > 0) | (z < 2) | (z + 1 == blks))
        def _():
            left_home(k)

    repeat(0, blks - 1, home)
    every = keys.at[pl.ds(0, 2 * chips - blks)]
    pltpu.make_async_copy(every, every, sent).wait()


def local(raw_desc, desc_mean, whitening):
    rows, depth = raw_desc.shape
    width = whitening.shape[1]
    blks, tiles = lax.axis_size("blk"), lax.axis_size("tile")
    chips = blks * tiles
    vmem = pl.BlockSpec(memory_space=pltpu.VMEM)
    hbm = pl.BlockSpec(memory_space=pltpu.HBM)
    dma = pltpu.SemaphoreType.DMA
    bf16, f32 = jnp.bfloat16, jnp.float32
    raw_desc = pltpu.with_memory_space_constraint(raw_desc, pltpu.HBM)
    desc_mean = pltpu.with_memory_space_constraint(desc_mean, pltpu.HBM)
    whitening = pltpu.with_memory_space_constraint(whitening, pltpu.HBM)
    return pl.pallas_call(
        functools.partial(kernel, blks, tiles),
        out_shape=jax.ShapeDtypeStruct((rows, width), f32),
        in_specs=[hbm, hbm, hbm],
        out_specs=vmem,
        scratch_shapes=[
            pltpu.VMEM((rows, depth), bf16),
            pltpu.VMEM((depth,), f32),
            pltpu.VMEM((depth, width), bf16),
            pltpu.VMEM((2 * chips, rows, width), bf16),
            pltpu.VMEM((rows, 2 * width), f32),
            pltpu.VMEM((2, rows, width), f32),
            dma((slabs,)),
            dma((slabs,)),
            dma,
            dma,
            dma((chips, pieces)),
            dma((chips,)),
            pltpu.SemaphoreType.REGULAR((blks - 1,)),
            pltpu.SemaphoreType.REGULAR((tiles - 1,)),
            dma((blks - 1,)),
            pltpu.SemaphoreType.REGULAR,
        ],
        compiler_params=pltpu.CompilerParams(collective_id=0, has_side_effects=True, vmem_limit_bytes=40 * 2 ** 20),
        name="augment",
    )(raw_desc, desc_mean, whitening)


def solution(mesh):
    return jax.shard_map(
        local,
        mesh=mesh,
        in_specs=(P(("groups", "blk", "tile"), None), P(), P(None, "sub")),
        out_specs=P(("groups", "blk", "tile"), "sub"),
        check_vma=False,
    )
```

```python
import functools

import jax
import jax.numpy as jnp
from jax import lax
from jax.experimental import pallas as pl
from jax.experimental.pallas import tpu as pltpu
from jax.sharding import PartitionSpec as P

beta = 0.125
lowest = -1e30
slabs = 3
pieces = 2
MESH = pl.DeviceIdType.MESH


def repeat(start, stop, body):
    if stop - start <= 8:
        for k in range(start, stop):
            body(k)
    else:
        lax.fori_loop(start, stop, lambda k, _: (body(k), 0)[1], 0)


def other_than(me, k):
    return k + jnp.where(k >= me, 1, 0)


def kernel(
    blks, tiles,
    raw_hbm, mean_hbm, white_hbm, out_ref,
    raw, mean, white, keys, query, feats, acc, best, total,
    raw_sem, white_sem, mean_sem, sent, recv, pair_recv, ready_z, ready_x, gone, turn, token,
):
    z, x, s = lax.axis_index("blk"), lax.axis_index("tile"), lax.axis_index("sub")
    other = 1 - s
    rows, width = keys.shape[1], keys.shape[2]
    chips = blks * tiles
    piece = rows // pieces
    slab = raw.shape[1] // slabs
    load_mean = pltpu.make_async_copy(mean_hbm, mean, mean_sem)
    load_mean.start()
    loads = []
    for c in range(slabs):
        at = pl.ds(c * slab, slab)
        loads.append((
            pltpu.make_async_copy(white_hbm.at[at], white.at[at], white_sem.at[c]),
            pltpu.make_async_copy(raw_hbm.at[:, at], raw.at[:, at], raw_sem.at[c]),
        ))
        for load in loads[-1]:
            load.start()

    barrier = pltpu.get_barrier_semaphore()

    def to_z(k):
        return {"blk": other_than(z, k)}

    def to_x(k):
        return {"tile": other_than(x, k)}

    def greet(device):
        pl.semaphore_signal(barrier, inc=1, device_id=device, device_id_type=MESH)

    greet({"sub": other})

    def greet_z(k):
        @pl.when(k >= z)
        def _():
            greet(to_z(k))

    def greet_x(k):
        @pl.when(k >= x)
        def _():
            greet(to_x(k))

    def answer_z(k):
        @pl.when(k < z)
        def _():
            pl.semaphore_signal(ready_z.at[z - 1], inc=1, device_id=to_z(k), device_id_type=MESH)

    def answer_x(k):
        @pl.when(k < x)
        def _():
            pl.semaphore_signal(ready_x.at[x - 1], inc=1, device_id=to_x(k), device_id_type=MESH)

    repeat(0, blks - 1, greet_z)
    repeat(0, tiles - 1, greet_x)
    pl.semaphore_wait(barrier, 1 + z + x)
    repeat(0, blks - 1, answer_z)
    repeat(0, tiles - 1, answer_x)

    def slot(zz, xx):
        return zz * tiles + xx

    mine = slot(z, x)

    def send(block, p, device, done=sent):
        at = keys.at[2 * block + s, pl.ds(p * piece, piece)]
        pltpu.make_async_remote_copy(
            at, at, done, recv.at[block, p], device_id=device, device_id_type=MESH,
        ).start()

    def left_home(k, p):
        at = keys.at[0, pl.ds(0, piece)]
        pltpu.make_async_copy(at, at, gone.at[k, p]).wait()

    def share(block, p):
        at = keys.at[2 * block + s, pl.ds(p * piece, piece)]
        pltpu.make_async_remote_copy(
            at, at, sent, pair_recv.at[block], device_id={"sub": other}, device_id_type=MESH,
        ).start()

    load_mean.wait()
    half = None
    for c in range(slabs):
        at = pl.ds(c * slab, slab)
        for load in loads[c]:
            load.wait()
        centred = (raw[:, at].astype(jnp.float32) - mean[at].reshape(1, -1)).astype(jnp.bfloat16)
        term = jnp.dot(centred, white[at, :], preferred_element_type=jnp.float32)
        half = term if half is None else half + term
    keys[2 * mine + s] = half.astype(jnp.bfloat16)
    def push(k):
        for p in range(pieces):
            send(mine, p, to_z(k), gone.at[k, p])

    def rightward(k):
        @pl.when(k >= z)
        def _():
            pl.semaphore_wait(ready_z.at[k], 1)
            push(k)

    def leftward(k):
        @pl.when(k < z - 1)
        def _():
            push(k)

    def sideward(k):
        @pl.when(k >= x)
        def _():
            pl.semaphore_wait(ready_x.at[k], 1)
        for p in range(pieces):
            send(mine, p, to_x(k))

    for p in range(pieces):
        share(mine, p)

    @pl.when(z > 0)
    def _():
        push(0)

    repeat(0, tiles - 1, sideward)
    repeat(0, blks - 1, rightward)

    @pl.when(z > 1)
    def _():
        left_home(0, 0)
        pl.semaphore_signal(turn, inc=1, device_id={"sub": other}, device_id_type=MESH)

        @pl.when(z + 1 < blks)
        def _():
            for r in range(2):
                pl.semaphore_signal(
                    token, inc=1, device_id={"blk": z + 1, "sub": r}, device_id_type=MESH,
                )
        pl.semaphore_wait(turn, 1)
        push(z - 1)

    @pl.when(z > 2)
    def _():
        pl.semaphore_wait(token, 2)
    repeat(1, blks - 1, leftward)

    def take(block, forward):
        for p in range(pieces):
            at = keys.at[2 * block + s, pl.ds(p * piece, piece)]
            pltpu.make_async_copy(at, at, recv.at[block, p]).wait()
            if forward:
                repeat(0, tiles - 1, lambda k: send(block, p, to_x(k)))
            share(block, p)

    def both(block):
        return jnp.concatenate([keys[2 * block], keys[2 * block + 1]], axis=1)

    def paired(block):
        at = keys.at[2 * block + other]
        pltpu.make_async_copy(at, at, pair_recv.at[block]).wait()

    def scores_of(kk):
        return jnp.dot(kk, query[...], preferred_element_type=jnp.float32)

    def weigh(kk, expo):
        tn = (((0,), (0,)), ((), ()))
        return lax.dot_general(
            kk, expo.astype(jnp.bfloat16), tn, preferred_element_type=jnp.float32
        )

    def folded(values):
        return jnp.sum(values.reshape(-1, 8, values.shape[1]), axis=0)

    def attend(*blocks):
        for block in blocks:
            paired(block)
        kk = jnp.concatenate([both(block) for block in blocks], axis=0)
        sc = scores_of(kk)
        old = best[...]
        top = jnp.maximum(old, jnp.max(sc, axis=0, keepdims=True))
        scale = jnp.exp(old - top)
        expo = jnp.exp(sc - top)
        best[...] = top
        total[...] = total[...] * scale + folded(expo)
        acc[...] = acc[...] * scale + weigh(kk, expo)

    paired(mine)
    own = both(mine)
    turned = own.astype(jnp.float32).T
    feats[...] = turned
    query[...] = (turned * beta).astype(jnp.bfloat16)
    sc = scores_of(own)
    key_at = lax.broadcasted_iota(jnp.int32, sc.shape, 0)
    query_at = lax.broadcasted_iota(jnp.int32, sc.shape, 1)
    masked = query_at == key_at
    sc = jnp.where(masked, lowest, sc)
    top = jnp.max(sc, axis=0, keepdims=True)
    expo = jnp.where(masked, 0.0, jnp.exp(sc - top))
    best[...] = top
    total[...] = folded(expo)
    acc[...] = weigh(own, expo)

    def nth(k):
        near = lax.rem(k + blks - 2, blks - 1)
        ahead = jnp.where(z == blks - 1, near, other_than(z, k))
        return jnp.where(z == 0, blks - 1 - k, ahead)

    def z_block(k):
        back = (z == 0) & (s == 0)
        near = lax.rem(k + blks - 2, blks - 1)
        ahead = jnp.where(z == blks - 1, near, other_than(z, k))
        return slot(jnp.where(back, blks - 1 - k, ahead), x)

    def x_block(k):
        return slot(z, other_than(x, k))

    def far_block(i):
        return slot(nth(i // (tiles - 1)), other_than(x, lax.rem(i, tiles - 1)))

    far = (blks - 1) * (tiles - 1)
    repeat(0, blks - 1, lambda k: take(z_block(k), True))
    repeat(0, tiles - 1, lambda k: take(x_block(k), False))
    if blks == 4 and tiles == 2:
        attend(slot(nth(0), x), slot(nth(1), x))
        attend(slot(nth(2), x), x_block(0))
        take(far_block(0), False)
        take(far_block(1), False)
        take(far_block(2), False)
        attend(far_block(0), far_block(1))
        attend(far_block(2))
    else:
        repeat(0, blks - 1, lambda k: attend(z_block(k)))
        repeat(0, tiles - 1, lambda k: attend(x_block(k)))
        take(far_block(0), False)

        def across(i):
            take(far_block(i), False)
            attend(far_block(i - 1))

        repeat(1, far, across)
        attend(far_block(far - 1))

    mixed = feats[...] + acc[...] * (1.0 / jnp.sum(total[...], axis=0, keepdims=True))
    squares = jnp.sum(mixed * mixed, axis=0, keepdims=True)
    wanted = jnp.where(s == 0, mixed[:width], mixed[width:])
    out_ref[...] = (wanted * lax.rsqrt(squares + 1e-06)).T

    def home(k):
        @pl.when((k > 0) | (z < 2))
        def _():
            left_home(k, 0)
        for p in range(1, pieces):
            left_home(k, p)

    repeat(0, blks - 1, home)
    every = keys.at[pl.ds(0, 2 * chips - blks)]
    pltpu.make_async_copy(every, every, sent).wait()


def local(raw_desc, desc_mean, whitening):
    rows, depth = raw_desc.shape
    width = whitening.shape[1]
    blks, tiles = lax.axis_size("blk"), lax.axis_size("tile")
    chips = blks * tiles
    vmem = pl.BlockSpec(memory_space=pltpu.VMEM)
    hbm = pl.BlockSpec(memory_space=pltpu.HBM)
    dma = pltpu.SemaphoreType.DMA
    bf16, f32 = jnp.bfloat16, jnp.float32
    raw_desc = pltpu.with_memory_space_constraint(raw_desc, pltpu.HBM)
    desc_mean = pltpu.with_memory_space_constraint(desc_mean, pltpu.HBM)
    whitening = pltpu.with_memory_space_constraint(whitening, pltpu.HBM)
    return pl.pallas_call(
        functools.partial(kernel, blks, tiles),
        out_shape=jax.ShapeDtypeStruct((rows, width), f32),
        in_specs=[hbm, hbm, hbm],
        out_specs=vmem,
        scratch_shapes=[
            pltpu.VMEM((rows, depth), bf16),
            pltpu.VMEM((depth,), f32),
            pltpu.VMEM((depth, width), bf16),
            pltpu.VMEM((2 * chips, rows, width), bf16),
            pltpu.VMEM((2 * width, rows), bf16),
            pltpu.VMEM((2 * width, rows), f32),
            pltpu.VMEM((2 * width, rows), f32),
            pltpu.VMEM((1, rows), f32),
            pltpu.VMEM((8, rows), f32),
            dma((slabs,)),
            dma((slabs,)),
            dma,
            dma,
            dma((chips, pieces)),
            dma((chips,)),
            pltpu.SemaphoreType.REGULAR((blks - 1,)),
            pltpu.SemaphoreType.REGULAR((tiles - 1,)),
            dma((blks - 1, pieces)),
            pltpu.SemaphoreType.REGULAR,
            pltpu.SemaphoreType.REGULAR,
        ],
        compiler_params=pltpu.CompilerParams(collective_id=0, has_side_effects=True, vmem_limit_bytes=40 * 2 ** 20),
        name="augment",
    )(raw_desc, desc_mean, whitening)


def solution(mesh):
    return jax.shard_map(
        local,
        mesh=mesh,
        in_specs=(P(("groups", "blk", "tile"), None), P(), P(None, "sub")),
        out_specs=P(("groups", "blk", "tile"), "sub"),
        check_vma=False,
    )
```

```python
import functools

import jax
import jax.numpy as jnp
from jax import lax
from jax.experimental import pallas as pl
from jax.experimental.pallas import tpu as pltpu
from jax.sharding import PartitionSpec as P

beta = 0.125
lowest = -1e30
slabs = 2
MESH = pl.DeviceIdType.MESH


def repeat(start, stop, body):
    if stop - start <= 8:
        for k in range(start, stop):
            body(k)
    else:
        lax.fori_loop(start, stop, lambda k, _: (body(k), 0)[1], 0)


def other_than(me, k):
    return k + jnp.where(k >= me, 1, 0)


def place(who, me):
    return who - jnp.where(who > me, 1, 0)


def kernel(
    blks, tiles,
    raw_hbm, mean_hbm, white_hbm, out_ref,
    raw, mean, white, keys, query, feats, acc, best, total,
    raw_sem, white_sem, mean_sem, sent, gone, recv, late, pair_recv, ready_z, ready_x, turn,
):
    z, x, s = lax.axis_index("blk"), lax.axis_index("tile"), lax.axis_index("sub")
    other = 1 - s
    rows, width = keys.shape[1], keys.shape[2]
    chips = blks * tiles
    piece = rows // 2
    slab = raw.shape[1] // slabs
    loads = []
    for c in range(slabs):
        at = pl.ds(c * slab, slab)
        loads.append(pltpu.make_async_copy(raw_hbm.at[:, at], raw.at[:, at], raw_sem.at[c]))
        loads[-1].start()
        if c == 0:
            load_mean = pltpu.make_async_copy(mean_hbm, mean, mean_sem)
            load_mean.start()
            load_white = pltpu.make_async_copy(white_hbm, white, white_sem)
            load_white.start()

    barrier = pltpu.get_barrier_semaphore()

    def signal(sem, device):
        pl.semaphore_signal(sem, inc=1, device_id=device, device_id_type=MESH)

    def to_z(k):
        return {"blk": other_than(z, k)}

    def to_x(k):
        return {"tile": other_than(x, k)}

    def greet_z(k):
        @pl.when(k >= z)
        def _():
            signal(barrier, to_z(k))

    def greet_x(k):
        @pl.when(k >= x)
        def _():
            signal(barrier, to_x(k))

    def answer_z(k):
        @pl.when(k < z)
        def _():
            signal(ready_z.at[z - 1], to_z(k))

    def answer_x(k):
        @pl.when(k < x)
        def _():
            signal(ready_x.at[x - 1], to_x(k))

    signal(barrier, {"sub": other})
    repeat(0, blks - 1, greet_z)
    repeat(0, tiles - 1, greet_x)
    pl.semaphore_wait(barrier, 1 + z + x)
    repeat(0, blks - 1, answer_z)
    repeat(0, tiles - 1, answer_x)

    def slot(zz, xx):
        return zz * tiles + xx

    mine = slot(z, x)

    def copy_to(at, done, arrived, device):
        pltpu.make_async_remote_copy(
            at, at, done, arrived, device_id=device, device_id_type=MESH,
        ).start()

    def part(block, p):
        return keys.at[2 * block + s, pl.ds(p * piece, piece)]

    def half(block):
        return keys.at[2 * block + s]

    def landed(at, sem):
        pltpu.make_async_copy(at, at, sem).wait()

    def centre(c):
        at = pl.ds(c * slab, slab)
        return (raw[:, at].astype(jnp.float32) - mean[at].reshape(1, -1)).astype(jnp.bfloat16)

    for c in range(slabs):
        loads[c].wait()
        if c == 0:
            load_mean.wait()
        if c == slabs - 1:
            load_white.wait()
        raw[:, pl.ds(c * slab, slab)] = centre(c)
    keys[2 * mine + s] = jnp.dot(
        raw[...], white[...], preferred_element_type=jnp.float32
    ).astype(jnp.bfloat16)

    def push(k, done=sent):
        dest = other_than(z, k)
        copy_to(part(mine, 0), done, recv.at[mine], {"blk": dest})
        copy_to(part(mine, 1), sent, late.at[place(z, dest)], {"blk": dest})

    def rightward(k):
        @pl.when(k >= z)
        def _():
            pl.semaphore_wait(ready_z.at[k], 1)
            push(k)

    def leftward(k):
        @pl.when(k < z - 1)
        def _():
            push(k)

    def sideward(k):
        @pl.when(k >= x)
        def _():
            pl.semaphore_wait(ready_x.at[k], 1)
        copy_to(half(mine), sent, recv.at[mine], to_x(k))

    for p in range(2):
        copy_to(part(mine, p), sent if p else gone, recv.at[mine], {"sub": other})

    @pl.when(z > 0)
    def _():
        push(0, gone)

    repeat(0, tiles - 1, sideward)

    @pl.when(z == 0)
    def _():
        pl.semaphore_wait(ready_z.at[0], 1)
        push(0, gone)

    repeat(1, blks - 1, rightward)

    @pl.when(z > 1)
    def _():
        landed(half(0), gone)
        signal(turn, {"sub": other})

        @pl.when(z + 1 < blks)
        def _():
            for r in range(2):
                signal(turn, {"blk": z + 1, "sub": r})
        pl.semaphore_wait(turn, jnp.where(z > 2, 3, 1))
        repeat(1, blks - 1, leftward)
        push(z - 1)

    def share(block, group):
        copy_to(half(block), sent, pair_recv.at[group], {"sub": other})

    def take_z(block, zz, group):
        for p in range(2):
            landed(part(block, p), late.at[place(zz, z)] if p else recv.at[block])
            repeat(0, tiles - 1, lambda k: copy_to(part(block, p), sent, recv.at[block], to_x(k)))
        share(block, group)

    def take(block, group):
        landed(half(block), recv.at[block])
        share(block, group)

    def both(block):
        return jnp.concatenate([keys[2 * block], keys[2 * block + 1]], axis=1)

    def paired(count, group):
        landed(keys.at[pl.ds(0, count)], pair_recv.at[group])

    def scores_of(kk):
        return jnp.dot(kk, query[...], preferred_element_type=jnp.float32)

    def weigh(kk, expo):
        tn = (((0,), (0,)), ((), ()))
        return lax.dot_general(
            kk, expo.astype(jnp.bfloat16), tn, preferred_element_type=jnp.float32
        )

    def folded(values):
        return jnp.sum(values.reshape(-1, 8, values.shape[1]), axis=0)

    def attend(*blocks):
        kk = jnp.concatenate([both(block) for block in blocks], axis=0)
        sc = scores_of(kk)
        old = best[...]
        top = jnp.maximum(old, jnp.max(sc, axis=0, keepdims=True))
        scale = jnp.exp(old - top)
        expo = jnp.exp(sc - top)
        best[...] = top
        total[...] = total[...] * scale + folded(expo)
        acc[...] = acc[...] * scale + weigh(kk, expo)

    landed(keys.at[2 * mine + other], recv.at[mine])
    own = both(mine)
    turned = own.astype(jnp.float32).T
    feats[...] = turned
    query[...] = (turned * beta).astype(jnp.bfloat16)
    sc = scores_of(own)
    key_at = lax.broadcasted_iota(jnp.int32, sc.shape, 0)
    query_at = lax.broadcasted_iota(jnp.int32, sc.shape, 1)
    masked = query_at == key_at
    sc = jnp.where(masked, lowest, sc)
    top = jnp.max(sc, axis=0, keepdims=True)
    expo = jnp.where(masked, 0.0, jnp.exp(sc - top))
    best[...] = top
    total[...] = folded(expo)
    acc[...] = weigh(own, expo)

    def nth(k):
        near = lax.rem(k + blks - 2, blks - 1)
        ahead = jnp.where(z == blks - 1, near, other_than(z, k))
        ahead = jnp.where((z == 1) & (k > 0), blks - k, ahead)
        return jnp.where(z == 0, blks - 1 - k, ahead)

    def z_take(k):
        zz = jnp.where((z == 0) & (s == 1), k + 1, nth(k))
        take_z(slot(zz, x), zz, 0)

    def x_block(k):
        return slot(z, other_than(x, k))

    def far_block(i):
        return slot(nth(i // (tiles - 1)), other_than(x, lax.rem(i, tiles - 1)))

    far = (blks - 1) * (tiles - 1)
    repeat(0, blks - 1, z_take)
    repeat(0, tiles - 1, lambda k: take(x_block(k), 0))
    if blks == 4 and tiles == 2:
        paired(4, 0)
        attend(*[slot(nth(k), x) for k in range(3)], x_block(0))
        take(far_block(0), 1)
        take(far_block(1), 1)
        take(far_block(2), 2)
        paired(2, 1)
        attend(far_block(0), far_block(1))
        paired(1, 2)
        attend(far_block(2))
    else:
        repeat(0, far, lambda i: take(far_block(i), 0))
        paired(chips - 1, 0)
        repeat(0, blks - 1, lambda k: attend(slot(nth(k), x)))
        repeat(0, tiles - 1, lambda k: attend(x_block(k)))
        repeat(0, far, lambda i: attend(far_block(i)))

    mixed = feats[...] + acc[...] * (1.0 / jnp.sum(total[...], axis=0, keepdims=True))
    squares = jnp.sum(mixed * mixed, axis=0, keepdims=True)
    wanted = jnp.where(s == 0, mixed[:width], mixed[width:])
    out_ref[...] = (wanted * lax.rsqrt(squares + 1e-06)).T

    @pl.when(z < 2)
    def _():
        landed(half(0), gone)
    landed(keys.at[pl.ds(0, 2 * chips - 2)], sent)


def local(raw_desc, desc_mean, whitening):
    rows, depth = raw_desc.shape
    width = whitening.shape[1]
    blks, tiles = lax.axis_size("blk"), lax.axis_size("tile")
    chips = blks * tiles
    vmem = pl.BlockSpec(memory_space=pltpu.VMEM)
    hbm = pl.BlockSpec(memory_space=pltpu.HBM)
    dma = pltpu.SemaphoreType.DMA
    regular = pltpu.SemaphoreType.REGULAR
    bf16, f32 = jnp.bfloat16, jnp.float32
    raw_desc = pltpu.with_memory_space_constraint(raw_desc, pltpu.HBM)
    desc_mean = pltpu.with_memory_space_constraint(desc_mean, pltpu.HBM)
    whitening = pltpu.with_memory_space_constraint(whitening, pltpu.HBM)
    return pl.pallas_call(
        functools.partial(kernel, blks, tiles),
        out_shape=jax.ShapeDtypeStruct((rows, width), f32),
        in_specs=[hbm, hbm, hbm],
        out_specs=vmem,
        scratch_shapes=[
            pltpu.VMEM((rows, depth), bf16),
            pltpu.VMEM((depth,), f32),
            pltpu.VMEM((depth, width), bf16),
            pltpu.VMEM((2 * chips, rows, width), bf16),
            pltpu.VMEM((2 * width, rows), bf16),
            pltpu.VMEM((2 * width, rows), f32),
            pltpu.VMEM((2 * width, rows), f32),
            pltpu.VMEM((1, rows), f32),
            pltpu.VMEM((8, rows), f32),
            dma((slabs,)),
            dma,
            dma,
            dma,
            dma,
            dma((chips,)),
            dma((blks - 1,)),
            dma((3,)),
            regular((blks - 1,)),
            regular((tiles - 1,)),
            regular,
        ],
        compiler_params=pltpu.CompilerParams(collective_id=0, has_side_effects=True, vmem_limit_bytes=40 * 2 ** 20),
        name="augment",
    )(raw_desc, desc_mean, whitening)


def solution(mesh):
    return jax.shard_map(
        local,
        mesh=mesh,
        in_specs=(P(("groups", "blk", "tile"), None), P(), P(None, "sub")),
        out_specs=P(("groups", "blk", "tile"), "sub"),
        check_vma=False,
    )
```

```python
import functools

import jax
import jax.numpy as jnp
from jax import lax
from jax.experimental import pallas as pl
from jax.experimental.pallas import tpu as pltpu
from jax.sharding import PartitionSpec as P

beta = 0.125
lowest = -1e30
slabs = 2
MESH = pl.DeviceIdType.MESH


def repeat(start, stop, body):
    if stop - start <= 8:
        for k in range(start, stop):
            body(k)
    else:
        lax.fori_loop(start, stop, lambda k, _: (body(k), 0)[1], 0)


def other_than(me, k):
    return k + jnp.where(k >= me, 1, 0)


def place(who, me):
    return who - jnp.where(who > me, 1, 0)


def kernel(
    blks, tiles,
    raw_hbm, mean_hbm, white_hbm, out_ref,
    raw, mean, white, keys, query, feats, acc, best, total,
    raw_sem, white_sem, mean_sem, sent, gone, recv, late, pair_recv, ready_z, ready_x, turn, last,
):
    z, x, s = lax.axis_index("blk"), lax.axis_index("tile"), lax.axis_index("sub")
    other = 1 - s
    rows, width = keys.shape[1], keys.shape[2]
    chips = blks * tiles
    paired_up = blks == 4 and tiles == 2
    piece = rows // 2
    slab = raw.shape[1] // slabs
    loads = []
    for c in range(slabs):
        at = pl.ds(c * slab, slab)
        loads.append(pltpu.make_async_copy(raw_hbm.at[:, at], raw.at[:, at], raw_sem.at[c]))
        loads[-1].start()
        if c == 0:
            load_mean = pltpu.make_async_copy(mean_hbm, mean, mean_sem)
            load_mean.start()
            load_white = pltpu.make_async_copy(white_hbm, white, white_sem)
            load_white.start()

    barrier = pltpu.get_barrier_semaphore()

    def signal(sem, device):
        pl.semaphore_signal(sem, inc=1, device_id=device, device_id_type=MESH)

    def to_z(k):
        return {"blk": other_than(z, k)}

    def to_x(k):
        return {"tile": other_than(x, k)}

    def greet_z(k):
        @pl.when(k >= z)
        def _():
            signal(barrier, to_z(k))

    def greet_x(k):
        @pl.when(k >= x)
        def _():
            signal(barrier, to_x(k))

    def answer_z(k):
        @pl.when(k < z)
        def _():
            signal(ready_z.at[z - 1], to_z(k))

    def answer_x(k):
        @pl.when(k < x)
        def _():
            signal(ready_x.at[x - 1], to_x(k))

    signal(barrier, {"sub": other})
    repeat(0, blks - 1, greet_z)
    repeat(0, tiles - 1, greet_x)
    pl.semaphore_wait(barrier, 1 + z + x)
    repeat(0, blks - 1, answer_z)
    repeat(0, tiles - 1, answer_x)

    def slot(zz, xx):
        return zz * tiles + xx

    mine = slot(z, x)

    def copy_to(at, done, arrived, device):
        pltpu.make_async_remote_copy(
            at, at, done, arrived, device_id=device, device_id_type=MESH,
        ).start()

    def part(block, p):
        return keys.at[2 * block + s, pl.ds(p * piece, piece)]

    def half(block):
        return keys.at[2 * block + s]

    def landed(at, sem):
        pltpu.make_async_copy(at, at, sem).wait()

    def centre(c):
        at = pl.ds(c * slab, slab)
        return (raw[:, at].astype(jnp.float32) - mean[at].reshape(1, -1)).astype(jnp.bfloat16)

    for c in range(slabs):
        loads[c].wait()
        if c == 0:
            load_mean.wait()
        if c == slabs - 1:
            load_white.wait()
        raw[:, pl.ds(c * slab, slab)] = centre(c)
    keys[2 * mine + s] = jnp.dot(
        raw[...], white[...], preferred_element_type=jnp.float32
    ).astype(jnp.bfloat16)

    def push(k, done=sent):
        dest = other_than(z, k)
        copy_to(part(mine, 0), done, recv.at[mine], {"blk": dest})
        copy_to(part(mine, 1), sent, late.at[place(z, dest)], {"blk": dest})

    def rightward(k):
        @pl.when(k >= z)
        def _():
            pl.semaphore_wait(ready_z.at[k], 1)
            push(k)

    def leftward(k):
        direct = (k < z - 1) & jnp.logical_not(paired_up & (s == 1))

        @pl.when(direct)
        def _():
            push(k)

    def sideward(k):
        @pl.when(k >= x)
        def _():
            pl.semaphore_wait(ready_x.at[k], 1)
        copy_to(half(mine), sent, recv.at[mine], to_x(k))

    for p in range(2):
        copy_to(part(mine, p), sent if p else gone, recv.at[mine], {"sub": other})

    @pl.when(z > 0)
    def _():
        push(0, gone)

    repeat(0, tiles - 1, sideward)

    @pl.when(z == 0)
    def _():
        pl.semaphore_wait(ready_z.at[0], 1)
        push(0, gone)

    repeat(1, blks - 1, rightward)

    @pl.when(z > 1)
    def _():
        landed(half(0), gone)
        signal(turn, {"sub": other})

        @pl.when(z + 1 < blks)
        def _():
            for r in range(2):
                signal(turn, {"blk": z + 1, "sub": r})
        pl.semaphore_wait(turn, jnp.where(z > 2, 3, 1))
        repeat(1, blks - 1, leftward)
        push(z - 1)

    def share(block, group):
        copy_to(half(block), sent, pair_recv.at[group], {"sub": other})

    def relay(block, zz, p):
        at = part(block, p)
        if not paired_up or p == 0:
            repeat(0, tiles - 1, lambda k: copy_to(at, sent, recv.at[block], to_x(k)))
            return
        final = zz == nth(blks - 2)

        @pl.when(final)
        def _():
            copy_to(at, sent, last, to_x(0))
            copy_to(at, sent, pair_recv.at[2], {"tile": other_than(x, 0), "sub": other})

        @pl.when(jnp.logical_not(final))
        def _():
            copy_to(at, sent, recv.at[block], to_x(0))

    def take_z(block, zz, group):
        for p in range(2):
            landed(part(block, p), late.at[place(zz, z)] if p else recv.at[block])
            relay(block, zz, p)
            if paired_up:
                arrived = late.at[place(zz, 1)] if p else recv.at[block]

                @pl.when((z == 0) & (s == 1) & (zz == blks - 1))
                def _():
                    copy_to(part(block, p), sent, arrived, {"blk": 1})
        share(block, group)

    def take_last(block):
        landed(part(block, 0), recv.at[block])
        copy_to(part(block, 0), sent, pair_recv.at[2], {"sub": other})
        landed(part(block, 1), last)

    def take(block, group):
        landed(half(block), recv.at[block])
        share(block, group)

    def both(block):
        return jnp.concatenate([keys[2 * block], keys[2 * block + 1]], axis=1)

    def paired(count, group):
        landed(keys.at[pl.ds(0, count)], pair_recv.at[group])

    def scores_of(kk):
        return jnp.dot(kk, query[...], preferred_element_type=jnp.float32)

    def weigh(kk, expo):
        tn = (((0,), (0,)), ((), ()))
        return lax.dot_general(
            kk, expo.astype(jnp.bfloat16), tn, preferred_element_type=jnp.float32
        )

    def folded(values):
        return jnp.sum(values.reshape(-1, 8, values.shape[1]), axis=0)

    def attend(*blocks):
        kk = jnp.concatenate([both(block) for block in blocks], axis=0)
        sc = scores_of(kk)
        old = best[...]
        top = jnp.maximum(old, jnp.max(sc, axis=0, keepdims=True))
        scale = jnp.exp(old - top)
        expo = jnp.exp(sc - top)
        best[...] = top
        total[...] = total[...] * scale + folded(expo)
        acc[...] = acc[...] * scale + weigh(kk, expo)

    landed(keys.at[2 * mine + other], recv.at[mine])
    own = both(mine)
    turned = own.astype(jnp.float32).T
    feats[...] = turned
    query[...] = (turned * beta).astype(jnp.bfloat16)
    sc = scores_of(own)
    key_at = lax.broadcasted_iota(jnp.int32, sc.shape, 0)
    query_at = lax.broadcasted_iota(jnp.int32, sc.shape, 1)
    masked = query_at == key_at
    sc = jnp.where(masked, lowest, sc)
    top = jnp.max(sc, axis=0, keepdims=True)
    expo = jnp.where(masked, 0.0, jnp.exp(sc - top))
    best[...] = top
    total[...] = folded(expo)
    acc[...] = weigh(own, expo)

    def nth(k):
        near = lax.rem(k + blks - 2, blks - 1)
        ahead = jnp.where(z == blks - 1, near, other_than(z, k))
        ahead = jnp.where((z == 1) & (k > 0), blks - k, ahead)
        return jnp.where(z == 0, blks - 1 - k, ahead)

    def z_take(k):
        zz = jnp.where((z <= 1) & (s == 1), other_than(z, k), nth(k))
        take_z(slot(zz, x), zz, 0)

    def x_block(k):
        return slot(z, other_than(x, k))

    def far_block(i):
        return slot(nth(i // (tiles - 1)), other_than(x, lax.rem(i, tiles - 1)))

    far = (blks - 1) * (tiles - 1)
    repeat(0, blks - 1, z_take)
    repeat(0, tiles - 1, lambda k: take(x_block(k), 0))
    if paired_up:
        def near_ones():
            paired(4, 0)
            attend(*[slot(nth(k), x) for k in range(3)], x_block(0))

        def first_far():
            paired(1, 1)
            attend(far_block(0))

        @pl.when(s == 0)
        def _():
            near_ones()
            take(far_block(0), 1)
            first_far()
            take(far_block(1), 2)
            take_last(far_block(2))

        @pl.when(s == 1)
        def _():
            take(far_block(0), 1)
            near_ones()
            take(far_block(1), 2)
            take_last(far_block(2))
            first_far()

        paired(2, 2)
        attend(far_block(1), far_block(2))
    else:
        repeat(0, far, lambda i: take(far_block(i), 0))
        paired(chips - 1, 0)
        repeat(0, blks - 1, lambda k: attend(slot(nth(k), x)))
        repeat(0, tiles - 1, lambda k: attend(x_block(k)))
        repeat(0, far, lambda i: attend(far_block(i)))

    mixed = feats[...] + acc[...] * (1.0 / jnp.sum(total[...], axis=0, keepdims=True))
    squares = jnp.sum(mixed * mixed, axis=0, keepdims=True)
    wanted = jnp.where(s == 0, mixed[:width], mixed[width:])
    out_ref[...] = (wanted * lax.rsqrt(squares + 1e-06)).T

    @pl.when(z < 2)
    def _():
        landed(half(0), gone)
    units = 2 * chips - 2
    if paired_up:
        more = (z == 0) & (s == 1)
        fewer = (z == blks - 1) & (s == 1)

        @pl.when(more)
        def _():
            landed(keys.at[pl.ds(0, units + 1)], sent)

        @pl.when(fewer)
        def _():
            landed(keys.at[pl.ds(0, units - 1)], sent)

        @pl.when(jnp.logical_not(more | fewer))
        def _():
            landed(keys.at[pl.ds(0, units)], sent)
    else:
        landed(keys.at[pl.ds(0, units)], sent)


def local(raw_desc, desc_mean, whitening):
    rows, depth = raw_desc.shape
    width = whitening.shape[1]
    blks, tiles = lax.axis_size("blk"), lax.axis_size("tile")
    chips = blks * tiles
    vmem = pl.BlockSpec(memory_space=pltpu.VMEM)
    hbm = pl.BlockSpec(memory_space=pltpu.HBM)
    dma = pltpu.SemaphoreType.DMA
    regular = pltpu.SemaphoreType.REGULAR
    bf16, f32 = jnp.bfloat16, jnp.float32
    raw_desc = pltpu.with_memory_space_constraint(raw_desc, pltpu.HBM)
    desc_mean = pltpu.with_memory_space_constraint(desc_mean, pltpu.HBM)
    whitening = pltpu.with_memory_space_constraint(whitening, pltpu.HBM)
    return pl.pallas_call(
        functools.partial(kernel, blks, tiles),
        out_shape=jax.ShapeDtypeStruct((rows, width), f32),
        in_specs=[hbm, hbm, hbm],
        out_specs=vmem,
        scratch_shapes=[
            pltpu.VMEM((rows, depth), bf16),
            pltpu.VMEM((depth,), f32),
            pltpu.VMEM((depth, width), bf16),
            pltpu.VMEM((2 * chips, rows, width), bf16),
            pltpu.VMEM((2 * width, rows), bf16),
            pltpu.VMEM((2 * width, rows), f32),
            pltpu.VMEM((2 * width, rows), f32),
            pltpu.VMEM((1, rows), f32),
            pltpu.VMEM((8, rows), f32),
            dma((slabs,)),
            dma,
            dma,
            dma,
            dma,
            dma((chips,)),
            dma((blks - 1,)),
            dma((3,)),
            regular((blks - 1,)),
            regular((tiles - 1,)),
            regular,
            dma,
        ],
        compiler_params=pltpu.CompilerParams(collective_id=0, has_side_effects=True, vmem_limit_bytes=40 * 2 ** 20),
        name="augment",
    )(raw_desc, desc_mean, whitening)


def solution(mesh):
    return jax.shard_map(
        local,
        mesh=mesh,
        in_specs=(P(("groups", "blk", "tile"), None), P(), P(None, "sub")),
        out_specs=P(("groups", "blk", "tile"), "sub"),
        check_vma=False,
    )
```

```python
import functools

import jax
import jax.numpy as jnp
from jax import lax
from jax.experimental import pallas as pl
from jax.experimental.pallas import tpu as pltpu
from jax.sharding import PartitionSpec as P

beta = 0.125
lowest = -1e30
slabs = 2
MESH = pl.DeviceIdType.MESH


def repeat(start, stop, body):
    if stop - start <= 8:
        for k in range(start, stop):
            body(k)
    else:
        lax.fori_loop(start, stop, lambda k, _: (body(k), 0)[1], 0)


def other_than(me, k):
    return k + jnp.where(k >= me, 1, 0)


def place(who, me):
    return who - jnp.where(who > me, 1, 0)


def kernel(
    blks, tiles,
    raw_hbm, mean_hbm, white_hbm, out_ref,
    raw, mean, white, keys, query, feats, acc, best, total,
    raw_sem, white_sem, mean_sem, sent, gone, recv, late, pair_recv, ready_z, ready_x, turn, last,
):
    z, x, s = lax.axis_index("blk"), lax.axis_index("tile"), lax.axis_index("sub")
    other = 1 - s
    rows, width = keys.shape[1], keys.shape[2]
    chips = blks * tiles
    paired_up = blks == 4 and tiles == 2
    piece = rows // 2
    cut = rows // 4
    slab = raw.shape[1] // slabs
    loads = []
    for c in range(slabs):
        at = pl.ds(c * slab, slab)
        loads.append(pltpu.make_async_copy(raw_hbm.at[:, at], raw.at[:, at], raw_sem.at[c]))
        loads[-1].start()
        if c == 0:
            load_mean = pltpu.make_async_copy(mean_hbm, mean, mean_sem)
            load_mean.start()
            load_white = pltpu.make_async_copy(white_hbm, white, white_sem)
            load_white.start()

    barrier = pltpu.get_barrier_semaphore()

    def signal(sem, device):
        pl.semaphore_signal(sem, inc=1, device_id=device, device_id_type=MESH)

    def to_z(k):
        return {"blk": other_than(z, k)}

    def to_x(k):
        return {"tile": other_than(x, k)}

    def greet_z(k):
        @pl.when(k >= z)
        def _():
            signal(barrier, to_z(k))

    def greet_x(k):
        @pl.when(k >= x)
        def _():
            signal(barrier, to_x(k))

    def answer_z(k):
        @pl.when(k < z)
        def _():
            signal(ready_z.at[z - 1], to_z(k))

    def answer_x(k):
        @pl.when(k < x)
        def _():
            signal(ready_x.at[x - 1], to_x(k))

    signal(barrier, {"sub": other})
    repeat(0, blks - 1, greet_z)
    repeat(0, tiles - 1, greet_x)
    pl.semaphore_wait(barrier, 1 + z + x)
    repeat(0, blks - 1, answer_z)
    repeat(0, tiles - 1, answer_x)

    def slot(zz, xx):
        return zz * tiles + xx

    mine = slot(z, x)

    def copy_to(at, done, arrived, device):
        pltpu.make_async_remote_copy(
            at, at, done, arrived, device_id=device, device_id_type=MESH,
        ).start()

    def part(block, p):
        return keys.at[2 * block + s, pl.ds(p * piece, piece)]

    def half(block):
        return keys.at[2 * block + s]

    def ends(block):
        at = keys.at[2 * block + s]
        return at.at[pl.ds(0, cut)], at.at[pl.ds(cut, rows - cut)]

    def landed(at, sem):
        pltpu.make_async_copy(at, at, sem).wait()

    def centre(c):
        at = pl.ds(c * slab, slab)
        return (raw[:, at].astype(jnp.float32) - mean[at].reshape(1, -1)).astype(jnp.bfloat16)

    for c in range(slabs):
        loads[c].wait()
        if c == 0:
            load_mean.wait()
        if c == slabs - 1:
            load_white.wait()
        raw[:, pl.ds(c * slab, slab)] = centre(c)
    keys[2 * mine + s] = jnp.dot(
        raw[...], white[...], preferred_element_type=jnp.float32
    ).astype(jnp.bfloat16)

    def push(k, done=sent):
        dest = other_than(z, k)
        copy_to(part(mine, 0), done, recv.at[mine], {"blk": dest})
        copy_to(part(mine, 1), sent, late.at[place(z, dest)], {"blk": dest})

    def rightward(k):
        @pl.when(k >= z)
        def _():
            pl.semaphore_wait(ready_z.at[k], 1)
            push(k)

    def leftward(k):
        direct = (k < z - 1) & jnp.logical_not(paired_up & (s == 1))

        @pl.when(direct)
        def _():
            push(k)

    def sideward(k):
        @pl.when(k >= x)
        def _():
            pl.semaphore_wait(ready_x.at[k], 1)
        copy_to(half(mine), sent, recv.at[mine], to_x(k))

    for p in range(2):
        copy_to(part(mine, p), sent if p else gone, recv.at[mine], {"sub": other})

    @pl.when(z > 0)
    def _():
        push(0, gone)

    repeat(0, tiles - 1, sideward)

    @pl.when(z == 0)
    def _():
        pl.semaphore_wait(ready_z.at[0], 1)
        push(0, gone)

    repeat(1, blks - 1, rightward)

    @pl.when(z > 1)
    def _():
        landed(half(0), gone)
        signal(turn, {"sub": other})

        @pl.when(z + 1 < blks)
        def _():
            for r in range(2):
                signal(turn, {"blk": z + 1, "sub": r})
        pl.semaphore_wait(turn, jnp.where(z > 2, 3, 1))
        repeat(1, blks - 1, leftward)
        push(z - 1)

    def share(block, group):
        copy_to(half(block), sent, pair_recv.at[group], {"sub": other})

    def relay(block, zz, p):
        at = part(block, p)
        if not paired_up:
            repeat(0, tiles - 1, lambda k: copy_to(at, sent, recv.at[block], to_x(k)))
            return
        final = (zz == nth(blks - 2)) & (s == 0)
        first, rest = ends(block)

        @pl.when(final)
        def _():
            if p == 0:
                copy_to(first, sent, recv.at[block], to_x(0))
            else:
                copy_to(rest, sent, last, to_x(0))
                across = {"tile": other_than(x, 0), "sub": other}
                copy_to(rest, sent, pair_recv.at[2], across)

        @pl.when(jnp.logical_not(final))
        def _():
            copy_to(at, sent, recv.at[block], to_x(0))

    def take_z(block, zz, group):
        for p in range(2):
            landed(part(block, p), late.at[place(zz, z)] if p else recv.at[block])
            relay(block, zz, p)
            if paired_up:
                arrived = late.at[place(zz, 1)] if p else recv.at[block]

                @pl.when((z == 0) & (s == 1) & (zz == blks - 1))
                def _():
                    copy_to(part(block, p), sent, arrived, {"blk": 1})
        share(block, group)

    def take_last(block):
        first, rest = ends(block)
        landed(first, recv.at[block])
        copy_to(first, sent, pair_recv.at[2], {"sub": other})
        landed(rest, last)

    def take(block, group):
        landed(half(block), recv.at[block])
        share(block, group)

    def both(block):
        return jnp.concatenate([keys[2 * block], keys[2 * block + 1]], axis=1)

    def paired(count, group):
        landed(keys.at[pl.ds(0, count)], pair_recv.at[group])

    def scores_of(kk):
        return jnp.dot(kk, query[...], preferred_element_type=jnp.float32)

    def weigh(kk, expo):
        tn = (((0,), (0,)), ((), ()))
        return lax.dot_general(
            kk, expo.astype(jnp.bfloat16), tn, preferred_element_type=jnp.float32
        )

    def folded(values):
        return jnp.sum(values.reshape(-1, 8, values.shape[1]), axis=0)

    def attend(*blocks):
        kk = jnp.concatenate([both(block) for block in blocks], axis=0)
        sc = scores_of(kk)
        old = best[...]
        top = jnp.maximum(old, jnp.max(sc, axis=0, keepdims=True))
        scale = jnp.exp(old - top)
        expo = jnp.exp(sc - top)
        best[...] = top
        total[...] = total[...] * scale + folded(expo)
        acc[...] = acc[...] * scale + weigh(kk, expo)

    landed(keys.at[2 * mine + other], recv.at[mine])
    own = both(mine)
    turned = own.astype(jnp.float32).T
    feats[...] = turned
    query[...] = (turned * beta).astype(jnp.bfloat16)
    sc = scores_of(own)
    key_at = lax.broadcasted_iota(jnp.int32, sc.shape, 0)
    query_at = lax.broadcasted_iota(jnp.int32, sc.shape, 1)
    masked = query_at == key_at
    sc = jnp.where(masked, lowest, sc)
    top = jnp.max(sc, axis=0, keepdims=True)
    expo = jnp.where(masked, 0.0, jnp.exp(sc - top))
    best[...] = top
    total[...] = folded(expo)
    acc[...] = weigh(own, expo)

    def nth(k):
        near = lax.rem(k + blks - 2, blks - 1)
        ahead = jnp.where(z == blks - 1, near, other_than(z, k))
        ahead = jnp.where((z == 1) & (k > 0), blks - k, ahead)
        return jnp.where(z == 0, blks - 1 - k, ahead)

    def z_take(k):
        zz = jnp.where((z <= 1) & (s == 1), other_than(z, k), nth(k))
        take_z(slot(zz, x), zz, 0)

    def x_block(k):
        return slot(z, other_than(x, k))

    def far_block(i):
        return slot(nth(i // (tiles - 1)), other_than(x, lax.rem(i, tiles - 1)))

    far = (blks - 1) * (tiles - 1)
    repeat(0, blks - 1, z_take)
    repeat(0, tiles - 1, lambda k: take(x_block(k), 0))
    if paired_up:
        def near_ones():
            paired(4, 0)
            attend(*[slot(nth(k), x) for k in range(3)], x_block(0))

        def first_far():
            paired(1, 1)
            attend(far_block(0))

        @pl.when(s == 0)
        def _():
            near_ones()
            take(far_block(0), 1)
            first_far()
            take(far_block(1), 2)
            take_last(far_block(2))

        @pl.when(s == 1)
        def _():
            take(far_block(0), 1)
            near_ones()
            take(far_block(1), 2)
            take(far_block(2), 2)
            first_far()

        paired(2, 2)
        attend(far_block(1), far_block(2))
    else:
        repeat(0, far, lambda i: take(far_block(i), 0))
        paired(chips - 1, 0)
        repeat(0, blks - 1, lambda k: attend(slot(nth(k), x)))
        repeat(0, tiles - 1, lambda k: attend(x_block(k)))
        repeat(0, far, lambda i: attend(far_block(i)))

    mixed = feats[...] + acc[...] * (1.0 / jnp.sum(total[...], axis=0, keepdims=True))
    squares = jnp.sum(mixed * mixed, axis=0, keepdims=True)
    wanted = jnp.where(s == 0, mixed[:width], mixed[width:])
    out_ref[...] = (wanted * lax.rsqrt(squares + 1e-06)).T

    @pl.when(z < 2)
    def _():
        landed(half(0), gone)
    units = 2 * chips - 2
    if paired_up:
        more = (z == 0) & (s == 1)
        fewer = (z == blks - 1) & (s == 1)

        @pl.when(more)
        def _():
            landed(keys.at[pl.ds(0, units + 1)], sent)

        @pl.when(fewer)
        def _():
            landed(keys.at[pl.ds(0, units - 1)], sent)

        @pl.when(jnp.logical_not(more | fewer))
        def _():
            landed(keys.at[pl.ds(0, units)], sent)
    else:
        landed(keys.at[pl.ds(0, units)], sent)


def local(raw_desc, desc_mean, whitening):
    rows, depth = raw_desc.shape
    width = whitening.shape[1]
    blks, tiles = lax.axis_size("blk"), lax.axis_size("tile")
    chips = blks * tiles
    vmem = pl.BlockSpec(memory_space=pltpu.VMEM)
    hbm = pl.BlockSpec(memory_space=pltpu.HBM)
    dma = pltpu.SemaphoreType.DMA
    regular = pltpu.SemaphoreType.REGULAR
    bf16, f32 = jnp.bfloat16, jnp.float32
    raw_desc = pltpu.with_memory_space_constraint(raw_desc, pltpu.HBM)
    desc_mean = pltpu.with_memory_space_constraint(desc_mean, pltpu.HBM)
    whitening = pltpu.with_memory_space_constraint(whitening, pltpu.HBM)
    return pl.pallas_call(
        functools.partial(kernel, blks, tiles),
        out_shape=jax.ShapeDtypeStruct((rows, width), f32),
        in_specs=[hbm, hbm, hbm],
        out_specs=vmem,
        scratch_shapes=[
            pltpu.VMEM((rows, depth), bf16),
            pltpu.VMEM((depth,), f32),
            pltpu.VMEM((depth, width), bf16),
            pltpu.VMEM((2 * chips, rows, width), bf16),
            pltpu.VMEM((2 * width, rows), bf16),
            pltpu.VMEM((2 * width, rows), f32),
            pltpu.VMEM((2 * width, rows), f32),
            pltpu.VMEM((1, rows), f32),
            pltpu.VMEM((8, rows), f32),
            dma((slabs,)),
            dma,
            dma,
            dma,
            dma,
            dma((chips,)),
            dma((blks - 1,)),
            dma((3,)),
            regular((blks - 1,)),
            regular((tiles - 1,)),
            regular,
            dma,
        ],
        compiler_params=pltpu.CompilerParams(collective_id=0, has_side_effects=True, vmem_limit_bytes=40 * 2 ** 20),
        name="augment",
    )(raw_desc, desc_mean, whitening)


def solution(mesh):
    return jax.shard_map(
        local,
        mesh=mesh,
        in_specs=(P(("groups", "blk", "tile"), None), P(), P(None, "sub")),
        out_specs=P(("groups", "blk", "tile"), "sub"),
        check_vma=False,
    )
```

```python
import functools

import jax
import jax.numpy as jnp
from jax import lax
from jax.experimental import pallas as pl
from jax.experimental.pallas import tpu as pltpu
from jax.sharding import PartitionSpec as P

beta = 0.125
lowest = -1e30
slabs = 2
MESH = pl.DeviceIdType.MESH


def repeat(start, stop, body):
    if stop - start <= 8:
        for k in range(start, stop):
            body(k)
    else:
        lax.fori_loop(start, stop, lambda k, _: (body(k), 0)[1], 0)


def other_than(me, k):
    return k + jnp.where(k >= me, 1, 0)


def place(who, me):
    return who - jnp.where(who > me, 1, 0)


def kernel(
    blks, tiles,
    raw_hbm, mean_hbm, white_hbm, out_ref,
    raw, mean, white, keys, query, feats, acc, best, total,
    raw_sem, white_sem, mean_sem, sent, gone, recv, late, pair_recv, ready_z, ready_x, turn, last,
):
    z, x, s = lax.axis_index("blk"), lax.axis_index("tile"), lax.axis_index("sub")
    other = 1 - s
    rows, width = keys.shape[1], keys.shape[2]
    chips = blks * tiles
    paired_up = blks == 4 and tiles == 2
    piece = rows // 2
    cut = rows // 4
    slab = raw.shape[1] // slabs
    loads = []
    for c in range(slabs):
        at = pl.ds(c * slab, slab)
        loads.append(pltpu.make_async_copy(raw_hbm.at[:, at], raw.at[:, at], raw_sem.at[c]))
        loads[-1].start()
        if c == 0:
            load_mean = pltpu.make_async_copy(mean_hbm, mean, mean_sem)
            load_mean.start()
            load_white = pltpu.make_async_copy(white_hbm, white, white_sem)
            load_white.start()

    barrier = pltpu.get_barrier_semaphore()

    def signal(sem, device):
        pl.semaphore_signal(sem, inc=1, device_id=device, device_id_type=MESH)

    def to_z(k):
        return {"blk": other_than(z, k)}

    def to_x(k):
        return {"tile": other_than(x, k)}

    def greet_z(k):
        @pl.when(k >= z)
        def _():
            signal(barrier, to_z(k))

    def greet_x(k):
        @pl.when(k >= x)
        def _():
            signal(barrier, to_x(k))

    def answer_z(k):
        @pl.when(k < z)
        def _():
            signal(ready_z.at[z - 1], to_z(k))

    def answer_x(k):
        @pl.when(k < x)
        def _():
            signal(ready_x.at[x - 1], to_x(k))

    corner = paired_up & (z == 1) & (x == 1) & (s == 0)
    signal(barrier, {"sub": other})

    @pl.when(paired_up & (z == 0) & (x == 0) & (s == 0))
    def _():
        signal(barrier, {"blk": 1, "tile": 1 if paired_up else 0})

    repeat(0, blks - 1, greet_z)
    repeat(0, tiles - 1, greet_x)
    pl.semaphore_wait(barrier, 1 + z + x + jnp.where(corner, 1, 0))
    repeat(0, blks - 1, answer_z)
    repeat(0, tiles - 1, answer_x)

    def slot(zz, xx):
        return zz * tiles + xx

    mine = slot(z, x)

    def copy_to(at, done, arrived, device):
        pltpu.make_async_remote_copy(
            at, at, done, arrived, device_id=device, device_id_type=MESH,
        ).start()

    def part(block, p):
        return keys.at[2 * block + s, pl.ds(p * piece, piece)]

    def half(block):
        return keys.at[2 * block + s]

    def ends(block):
        at = keys.at[2 * block + s]
        return at.at[pl.ds(0, cut)], at.at[pl.ds(cut, rows - cut)]

    def landed(at, sem):
        pltpu.make_async_copy(at, at, sem).wait()

    def centre(c):
        at = pl.ds(c * slab, slab)
        return (raw[:, at].astype(jnp.float32) - mean[at].reshape(1, -1)).astype(jnp.bfloat16)

    for c in range(slabs):
        loads[c].wait()
        if c == 0:
            load_mean.wait()
        if c == slabs - 1:
            load_white.wait()
        raw[:, pl.ds(c * slab, slab)] = centre(c)
    keys[2 * mine + s] = jnp.dot(
        raw[...], white[...], preferred_element_type=jnp.float32
    ).astype(jnp.bfloat16)

    def push(k, done=sent):
        dest = other_than(z, k)
        copy_to(part(mine, 0), done, recv.at[mine], {"blk": dest})
        copy_to(part(mine, 1), sent, late.at[place(z, dest)], {"blk": dest})

    def rightward(k):
        @pl.when(k >= z)
        def _():
            pl.semaphore_wait(ready_z.at[k], 1)
            push(k)

    def leftward(k):
        direct = (k < z - 1) & jnp.logical_not(paired_up & (s == 1))

        @pl.when(direct)
        def _():
            push(k)

    def sideward(k):
        @pl.when(k >= x)
        def _():
            pl.semaphore_wait(ready_x.at[k], 1)
        copy_to(half(mine), sent, recv.at[mine], to_x(k))

    for p in range(2):
        copy_to(part(mine, p), sent if p else gone, recv.at[mine], {"sub": other})

    @pl.when(z > 0)
    def _():
        push(0, gone)

    @pl.when(corner)
    def _():
        copy_to(half(mine), sent, recv.at[mine], {"blk": 0, "tile": 0})

    repeat(0, tiles - 1, sideward)

    @pl.when(z == 0)
    def _():
        pl.semaphore_wait(ready_z.at[0], 1)
        push(0, gone)

    repeat(1, blks - 1, rightward)

    @pl.when(z > 1)
    def _():
        landed(half(0), gone)
        signal(turn, {"sub": other})

        @pl.when(z + 1 < blks)
        def _():
            for r in range(2):
                signal(turn, {"blk": z + 1, "sub": r})
        pl.semaphore_wait(turn, jnp.where(z > 2, 3, 1))
        repeat(1, blks - 1, leftward)
        push(z - 1)

    def share(block, group):
        copy_to(half(block), sent, pair_recv.at[group], {"sub": other})

    def relay(block, zz, p):
        at = part(block, p)
        if not paired_up:
            repeat(0, tiles - 1, lambda k: copy_to(at, sent, recv.at[block], to_x(k)))
            return
        final = (zz == nth(blks - 2, other_than(x, 0))) & (s == 0)
        spared = (z == 0) & (x == 1) & (s == 0)
        first, rest = ends(block)

        @pl.when(final)
        def _():
            if p == 0:
                copy_to(first, sent, recv.at[block], to_x(0))
            else:
                copy_to(rest, sent, last, to_x(0))
                across = {"tile": other_than(x, 0), "sub": other}
                copy_to(rest, sent, pair_recv.at[2], across)

        @pl.when(jnp.logical_not(final | (spared & (zz == 1))))
        def _():
            copy_to(at, sent, recv.at[block], to_x(0))

    def take_z(block, zz, group):
        for p in range(2):
            landed(part(block, p), late.at[place(zz, z)] if p else recv.at[block])
            relay(block, zz, p)
            if paired_up:
                arrived = late.at[place(zz, 1)] if p else recv.at[block]

                @pl.when((z == 0) & (s == 1) & (zz == blks - 1))
                def _():
                    copy_to(part(block, p), sent, arrived, {"blk": 1})
        share(block, group)

    def take_last(block):
        first, rest = ends(block)
        landed(first, recv.at[block])
        copy_to(first, sent, pair_recv.at[2], {"sub": other})
        landed(rest, last)

    def take(block, group):
        landed(half(block), recv.at[block])
        share(block, group)

    def both(block):
        return jnp.concatenate([keys[2 * block], keys[2 * block + 1]], axis=1)

    def paired(count, group):
        landed(keys.at[pl.ds(0, count)], pair_recv.at[group])

    def scores_of(kk):
        return jnp.dot(kk, query[...], preferred_element_type=jnp.float32)

    def weigh(kk, expo):
        tn = (((0,), (0,)), ((), ()))
        return lax.dot_general(
            kk, expo.astype(jnp.bfloat16), tn, preferred_element_type=jnp.float32
        )

    def folded(values):
        return jnp.sum(values.reshape(-1, 8, values.shape[1]), axis=0)

    def attend(*blocks):
        kk = jnp.concatenate([both(block) for block in blocks], axis=0)
        sc = scores_of(kk)
        old = best[...]
        top = jnp.maximum(old, jnp.max(sc, axis=0, keepdims=True))
        scale = jnp.exp(old - top)
        expo = jnp.exp(sc - top)
        best[...] = top
        total[...] = total[...] * scale + folded(expo)
        acc[...] = acc[...] * scale + weigh(kk, expo)

    landed(keys.at[2 * mine + other], recv.at[mine])
    own = both(mine)
    turned = own.astype(jnp.float32).T
    feats[...] = turned
    query[...] = (turned * beta).astype(jnp.bfloat16)
    sc = scores_of(own)
    key_at = lax.broadcasted_iota(jnp.int32, sc.shape, 0)
    query_at = lax.broadcasted_iota(jnp.int32, sc.shape, 1)
    masked = query_at == key_at
    sc = jnp.where(masked, lowest, sc)
    top = jnp.max(sc, axis=0, keepdims=True)
    expo = jnp.where(masked, 0.0, jnp.exp(sc - top))
    best[...] = top
    total[...] = folded(expo)
    acc[...] = weigh(own, expo)

    def nth(k, xx=x):
        near = lax.rem(k + blks - 2, blks - 1)
        ahead = jnp.where(z == blks - 1, near, other_than(z, k))
        ahead = jnp.where((z == 1) & (k > 0), blks - k, ahead)
        corner_first = jnp.where(k == 0, 1, blks - k)
        down = blks - 1 - k
        return jnp.where(z == 0, jnp.where(xx == 0, corner_first, down), ahead)

    def z_take(k):
        back = jnp.where(z == 0, blks - 1 - k, nth(k))
        zz = jnp.where((z <= 1) & (s == 1), other_than(z, k), back)
        take_z(slot(zz, x), zz, 0)

    def x_block(k):
        return slot(z, other_than(x, k))

    def far_block(i):
        return slot(nth(i // (tiles - 1)), other_than(x, lax.rem(i, tiles - 1)))

    far = (blks - 1) * (tiles - 1)
    repeat(0, blks - 1, z_take)
    repeat(0, tiles - 1, lambda k: take(x_block(k), 0))
    if paired_up:
        def near_ones():
            paired(4, 0)
            attend(*[slot(nth(k), x) for k in range(3)], x_block(0))

        def first_far():
            paired(1, 1)
            attend(far_block(0))

        @pl.when(s == 0)
        def _():
            near_ones()
            take(far_block(0), 1)
            first_far()
            take(far_block(1), 2)
            take_last(far_block(2))

        @pl.when(s == 1)
        def _():
            take(far_block(0), 1)
            near_ones()
            take(far_block(1), 2)
            take(far_block(2), 2)
            first_far()

        paired(2, 2)
        attend(far_block(1), far_block(2))
    else:
        repeat(0, far, lambda i: take(far_block(i), 0))
        paired(chips - 1, 0)
        repeat(0, blks - 1, lambda k: attend(slot(nth(k), x)))
        repeat(0, tiles - 1, lambda k: attend(x_block(k)))
        repeat(0, far, lambda i: attend(far_block(i)))

    mixed = feats[...] + acc[...] * (1.0 / jnp.sum(total[...], axis=0, keepdims=True))
    squares = jnp.sum(mixed * mixed, axis=0, keepdims=True)
    wanted = jnp.where(s == 0, mixed[:width], mixed[width:])
    out_ref[...] = (wanted * lax.rsqrt(squares + 1e-06)).T

    @pl.when(z < 2)
    def _():
        landed(half(0), gone)
    units = 2 * chips - 2
    if paired_up:
        more = ((z == 0) & (s == 1)) | corner
        fewer = ((z == blks - 1) & (s == 1)) | ((z == 0) & (x == 1) & (s == 0))

        @pl.when(more)
        def _():
            landed(keys.at[pl.ds(0, units + 1)], sent)

        @pl.when(fewer)
        def _():
            landed(keys.at[pl.ds(0, units - 1)], sent)

        @pl.when(jnp.logical_not(more | fewer))
        def _():
            landed(keys.at[pl.ds(0, units)], sent)
    else:
        landed(keys.at[pl.ds(0, units)], sent)


def local(raw_desc, desc_mean, whitening):
    rows, depth = raw_desc.shape
    width = whitening.shape[1]
    blks, tiles = lax.axis_size("blk"), lax.axis_size("tile")
    chips = blks * tiles
    vmem = pl.BlockSpec(memory_space=pltpu.VMEM)
    hbm = pl.BlockSpec(memory_space=pltpu.HBM)
    dma = pltpu.SemaphoreType.DMA
    regular = pltpu.SemaphoreType.REGULAR
    bf16, f32 = jnp.bfloat16, jnp.float32
    raw_desc = pltpu.with_memory_space_constraint(raw_desc, pltpu.HBM)
    desc_mean = pltpu.with_memory_space_constraint(desc_mean, pltpu.HBM)
    whitening = pltpu.with_memory_space_constraint(whitening, pltpu.HBM)
    return pl.pallas_call(
        functools.partial(kernel, blks, tiles),
        out_shape=jax.ShapeDtypeStruct((rows, width), f32),
        in_specs=[hbm, hbm, hbm],
        out_specs=vmem,
        scratch_shapes=[
            pltpu.VMEM((rows, depth), bf16),
            pltpu.VMEM((depth,), f32),
            pltpu.VMEM((depth, width), bf16),
            pltpu.VMEM((2 * chips, rows, width), bf16),
            pltpu.VMEM((2 * width, rows), bf16),
            pltpu.VMEM((2 * width, rows), f32),
            pltpu.VMEM((2 * width, rows), f32),
            pltpu.VMEM((1, rows), f32),
            pltpu.VMEM((8, rows), f32),
            dma((slabs,)),
            dma,
            dma,
            dma,
            dma,
            dma((chips,)),
            dma((blks - 1,)),
            dma((3,)),
            regular((blks - 1,)),
            regular((tiles - 1,)),
            regular,
            dma,
        ],
        compiler_params=pltpu.CompilerParams(collective_id=0, has_side_effects=True, vmem_limit_bytes=40 * 2 ** 20),
        name="augment",
    )(raw_desc, desc_mean, whitening)


def solution(mesh):
    return jax.shard_map(
        local,
        mesh=mesh,
        in_specs=(P(("groups", "blk", "tile"), None), P(), P(None, "sub")),
        out_specs=P(("groups", "blk", "tile"), "sub"),
        check_vma=False,
    )
```

```python
import functools

import jax
import jax.numpy as jnp
from jax import lax
from jax.experimental import pallas as pl
from jax.experimental.pallas import tpu as pltpu
from jax.sharding import PartitionSpec as P

beta = 0.125
lowest = -1e30
slabs = 2
MESH = pl.DeviceIdType.MESH


def repeat(start, stop, body):
    if stop - start <= 8:
        for k in range(start, stop):
            body(k)
    else:
        lax.fori_loop(start, stop, lambda k, _: (body(k), 0)[1], 0)


def other_than(me, k):
    return k + jnp.where(k >= me, 1, 0)


def place(who, me):
    return who - jnp.where(who > me, 1, 0)


def kernel(
    blks, tiles,
    raw_hbm, mean_hbm, white_hbm, out_ref,
    raw, mean, white, keys, query, feats, acc, best, total,
    raw_sem, white_sem, mean_sem, sent, gone, recv, late, pair_recv, ready_z, ready_x, turn, last,
):
    z, x, s = lax.axis_index("blk"), lax.axis_index("tile"), lax.axis_index("sub")
    other = 1 - s
    rows, width = keys.shape[1], keys.shape[2]
    chips = blks * tiles
    paired_up = blks == 4 and tiles == 2
    piece = rows // 2
    cut = rows // 4
    slab = raw.shape[1] // slabs
    loads = []
    for c in range(slabs):
        at = pl.ds(c * slab, slab)
        loads.append(pltpu.make_async_copy(raw_hbm.at[:, at], raw.at[:, at], raw_sem.at[c]))
        loads[-1].start()
        if c == 0:
            load_mean = pltpu.make_async_copy(mean_hbm, mean, mean_sem)
            load_mean.start()
            load_white = pltpu.make_async_copy(white_hbm, white, white_sem)
            load_white.start()

    barrier = pltpu.get_barrier_semaphore()

    def signal(sem, device):
        pl.semaphore_signal(sem, inc=1, device_id=device, device_id_type=MESH)

    def to_z(k):
        return {"blk": other_than(z, k)}

    def to_x(k):
        return {"tile": other_than(x, k)}

    def greet_z(k):
        @pl.when(k >= z)
        def _():
            signal(barrier, to_z(k))

    def greet_x(k):
        @pl.when(k >= x)
        def _():
            signal(barrier, to_x(k))

    def answer_z(k):
        @pl.when(k < z)
        def _():
            signal(ready_z.at[z - 1], to_z(k))

    def answer_x(k):
        @pl.when(k < x)
        def _():
            signal(ready_x.at[x - 1], to_x(k))

    corner = paired_up & (z == 1) & (x == 1) & (s == 0)
    signal(barrier, {"sub": other})

    @pl.when(paired_up & (z == 0) & (x == 0) & (s == 0))
    def _():
        signal(barrier, {"blk": 1, "tile": 1 if paired_up else 0})

    repeat(0, blks - 1, greet_z)
    repeat(0, tiles - 1, greet_x)
    pl.semaphore_wait(barrier, 1 + z + x + jnp.where(corner, 1, 0))
    repeat(0, blks - 1, answer_z)
    repeat(0, tiles - 1, answer_x)

    def slot(zz, xx):
        return zz * tiles + xx

    mine = slot(z, x)

    def copy_to(at, done, arrived, device):
        pltpu.make_async_remote_copy(
            at, at, done, arrived, device_id=device, device_id_type=MESH,
        ).start()

    def part(block, p):
        return keys.at[2 * block + s, pl.ds(p * piece, piece)]

    def half(block):
        return keys.at[2 * block + s]

    def ends(block):
        at = keys.at[2 * block + s]
        return at.at[pl.ds(0, cut)], at.at[pl.ds(cut, rows - cut)]

    def landed(at, sem):
        pltpu.make_async_copy(at, at, sem).wait()

    def centre(c):
        at = pl.ds(c * slab, slab)
        return (raw[:, at].astype(jnp.float32) - mean[at].reshape(1, -1)).astype(jnp.bfloat16)

    for c in range(slabs):
        loads[c].wait()
        if c == 0:
            load_mean.wait()
        if c == slabs - 1:
            load_white.wait()
        raw[:, pl.ds(c * slab, slab)] = centre(c)
    keys[2 * mine + s] = jnp.dot(
        raw[...], white[...], preferred_element_type=jnp.float32
    ).astype(jnp.bfloat16)

    def push(k, done=sent):
        dest = other_than(z, k)
        copy_to(part(mine, 0), done, recv.at[mine], {"blk": dest})
        copy_to(part(mine, 1), sent, late.at[place(z, dest)], {"blk": dest})

    def rightward(k):
        @pl.when(k >= z)
        def _():
            pl.semaphore_wait(ready_z.at[k], 1)
            push(k)

    def leftward(k):
        direct = (k < z - 1) & jnp.logical_not(paired_up & (s == 1))

        @pl.when(direct)
        def _():
            push(k)

    def sideward(k):
        @pl.when(k >= x)
        def _():
            pl.semaphore_wait(ready_x.at[k], 1)
        copy_to(half(mine), sent, recv.at[mine], to_x(k))

    for p in range(2):
        copy_to(part(mine, p), sent if p else gone, recv.at[mine], {"sub": other})

    @pl.when(z > 0)
    def _():
        push(0, gone)

    @pl.when(corner)
    def _():
        copy_to(half(mine), sent, recv.at[mine], {"blk": 0, "tile": 0})

    repeat(0, tiles - 1, sideward)

    @pl.when(z == 0)
    def _():
        pl.semaphore_wait(ready_z.at[0], 1)
        push(0, gone)

    repeat(1, blks - 1, rightward)

    @pl.when(z > 1)
    def _():
        landed(half(0), gone)
        @pl.when(z > 2)
        def _():
            signal(turn, {"sub": other})

        @pl.when(z + 1 < blks)
        def _():
            for r in range(2):
                signal(turn, {"blk": z + 1, "sub": r})
        @pl.when(z > 2)
        def _():
            pl.semaphore_wait(turn, 3)
        repeat(1, blks - 1, leftward)
        push(z - 1)

    def share(block, group):
        copy_to(half(block), sent, pair_recv.at[group], {"sub": other})

    def relay(block, zz, p):
        at = part(block, p)
        if not paired_up:
            repeat(0, tiles - 1, lambda k: copy_to(at, sent, recv.at[block], to_x(k)))
            return
        final = (zz == nth(blks - 2, other_than(x, 0))) & (s == 0)
        spared = (z == 0) & (x == 1) & (s == 0)
        first, rest = ends(block)

        @pl.when(final)
        def _():
            if p == 0:
                copy_to(first, sent, recv.at[block], to_x(0))
            else:
                copy_to(rest, sent, last, to_x(0))
                across = {"tile": other_than(x, 0), "sub": other}
                copy_to(rest, sent, pair_recv.at[2], across)

        @pl.when(jnp.logical_not(final | (spared & (zz == 1))))
        def _():
            copy_to(at, sent, recv.at[block], to_x(0))

    def take_z(block, zz, group):
        for p in range(2):
            landed(part(block, p), late.at[place(zz, z)] if p else recv.at[block])
            relay(block, zz, p)
            if paired_up:
                arrived = late.at[place(zz, 1)] if p else recv.at[block]

                @pl.when((z == 0) & (s == 1) & (zz == blks - 1))
                def _():
                    copy_to(part(block, p), sent, arrived, {"blk": 1})
        share(block, group)

    def take_last(block):
        first, rest = ends(block)
        landed(first, recv.at[block])
        copy_to(first, sent, pair_recv.at[2], {"sub": other})
        landed(rest, last)

    def take(block, group):
        landed(half(block), recv.at[block])
        share(block, group)

    def both(block):
        return jnp.concatenate([keys[2 * block], keys[2 * block + 1]], axis=1)

    def paired(count, group):
        landed(keys.at[pl.ds(0, count)], pair_recv.at[group])

    def scores_of(kk):
        return jnp.dot(kk, query[...], preferred_element_type=jnp.float32)

    def weigh(kk, expo):
        tn = (((0,), (0,)), ((), ()))
        return lax.dot_general(
            kk, expo.astype(jnp.bfloat16), tn, preferred_element_type=jnp.float32
        )

    def folded(values):
        return jnp.sum(values.reshape(-1, 8, values.shape[1]), axis=0)

    def attend(*blocks):
        kk = jnp.concatenate([both(block) for block in blocks], axis=0)
        sc = scores_of(kk)
        old = best[...]
        top = jnp.maximum(old, jnp.max(sc, axis=0, keepdims=True))
        scale = jnp.exp(old - top)
        expo = jnp.exp(sc - top)
        best[...] = top
        total[...] = total[...] * scale + folded(expo)
        acc[...] = acc[...] * scale + weigh(kk, expo)

    landed(keys.at[2 * mine + other], recv.at[mine])
    own = both(mine)
    turned = own.astype(jnp.float32).T
    feats[...] = turned
    query[...] = (turned * beta).astype(jnp.bfloat16)
    sc = scores_of(own)
    key_at = lax.broadcasted_iota(jnp.int32, sc.shape, 0)
    query_at = lax.broadcasted_iota(jnp.int32, sc.shape, 1)
    masked = query_at == key_at
    sc = jnp.where(masked, lowest, sc)
    top = jnp.max(sc, axis=0, keepdims=True)
    expo = jnp.where(masked, 0.0, jnp.exp(sc - top))
    best[...] = top
    total[...] = folded(expo)
    acc[...] = weigh(own, expo)

    def nth(k, xx=x):
        near = lax.rem(k + blks - 2, blks - 1)
        ahead = jnp.where(z == blks - 1, near, other_than(z, k))
        ahead = jnp.where((z == 1) & (k > 0), blks - k, ahead)
        corner_first = jnp.where(k == 0, 1, blks - k)
        down = blks - 1 - k
        return jnp.where(z == 0, jnp.where(xx == 0, corner_first, down), ahead)

    def z_take(k):
        back = jnp.where(z == 0, blks - 1 - k, nth(k))
        zz = jnp.where((z <= 1) & (s == 1), other_than(z, k), back)
        take_z(slot(zz, x), zz, 0)

    def x_block(k):
        return slot(z, other_than(x, k))

    def far_block(i):
        return slot(nth(i // (tiles - 1)), other_than(x, lax.rem(i, tiles - 1)))

    far = (blks - 1) * (tiles - 1)
    repeat(0, blks - 1, z_take)
    repeat(0, tiles - 1, lambda k: take(x_block(k), 0))
    if paired_up:
        def near_ones():
            paired(4, 0)
            attend(*[slot(nth(k), x) for k in range(3)], x_block(0))

        def first_far():
            paired(1, 1)
            attend(far_block(0))

        @pl.when(s == 0)
        def _():
            near_ones()
            take(far_block(0), 1)
            first_far()
            take(far_block(1), 2)
            take_last(far_block(2))

        @pl.when(s == 1)
        def _():
            take(far_block(0), 1)
            near_ones()
            take(far_block(1), 2)
            take(far_block(2), 2)
            first_far()

        paired(2, 2)
        attend(far_block(1), far_block(2))
    else:
        repeat(0, far, lambda i: take(far_block(i), 0))
        paired(chips - 1, 0)
        repeat(0, blks - 1, lambda k: attend(slot(nth(k), x)))
        repeat(0, tiles - 1, lambda k: attend(x_block(k)))
        repeat(0, far, lambda i: attend(far_block(i)))

    mixed = feats[...] + acc[...] * (1.0 / jnp.sum(total[...], axis=0, keepdims=True))
    squares = jnp.sum(mixed * mixed, axis=0, keepdims=True)
    wanted = jnp.where(s == 0, mixed[:width], mixed[width:])
    out_ref[...] = (wanted * lax.rsqrt(squares + 1e-06)).T

    @pl.when(z < 2)
    def _():
        landed(half(0), gone)
    units = 2 * chips - 2
    if paired_up:
        more = ((z == 0) & (s == 1)) | corner
        fewer = ((z == blks - 1) & (s == 1)) | ((z == 0) & (x == 1) & (s == 0))

        @pl.when(more)
        def _():
            landed(keys.at[pl.ds(0, units + 1)], sent)

        @pl.when(fewer)
        def _():
            landed(keys.at[pl.ds(0, units - 1)], sent)

        @pl.when(jnp.logical_not(more | fewer))
        def _():
            landed(keys.at[pl.ds(0, units)], sent)
    else:
        landed(keys.at[pl.ds(0, units)], sent)


def local(raw_desc, desc_mean, whitening):
    rows, depth = raw_desc.shape
    width = whitening.shape[1]
    blks, tiles = lax.axis_size("blk"), lax.axis_size("tile")
    chips = blks * tiles
    vmem = pl.BlockSpec(memory_space=pltpu.VMEM)
    hbm = pl.BlockSpec(memory_space=pltpu.HBM)
    dma = pltpu.SemaphoreType.DMA
    regular = pltpu.SemaphoreType.REGULAR
    bf16, f32 = jnp.bfloat16, jnp.float32
    raw_desc = pltpu.with_memory_space_constraint(raw_desc, pltpu.HBM)
    desc_mean = pltpu.with_memory_space_constraint(desc_mean, pltpu.HBM)
    whitening = pltpu.with_memory_space_constraint(whitening, pltpu.HBM)
    return pl.pallas_call(
        functools.partial(kernel, blks, tiles),
        out_shape=jax.ShapeDtypeStruct((rows, width), f32),
        in_specs=[hbm, hbm, hbm],
        out_specs=vmem,
        scratch_shapes=[
            pltpu.VMEM((rows, depth), bf16),
            pltpu.VMEM((depth,), f32),
            pltpu.VMEM((depth, width), bf16),
            pltpu.VMEM((2 * chips, rows, width), bf16),
            pltpu.VMEM((2 * width, rows), bf16),
            pltpu.VMEM((2 * width, rows), f32),
            pltpu.VMEM((2 * width, rows), f32),
            pltpu.VMEM((1, rows), f32),
            pltpu.VMEM((8, rows), f32),
            dma((slabs,)),
            dma,
            dma,
            dma,
            dma,
            dma((chips,)),
            dma((blks - 1,)),
            dma((3,)),
            regular((blks - 1,)),
            regular((tiles - 1,)),
            regular,
            dma,
        ],
        compiler_params=pltpu.CompilerParams(collective_id=0, has_side_effects=True, vmem_limit_bytes=40 * 2 ** 20),
        name="augment",
    )(raw_desc, desc_mean, whitening)


def solution(mesh):
    return jax.shard_map(
        local,
        mesh=mesh,
        in_specs=(P(("groups", "blk", "tile"), None), P(), P(None, "sub")),
        out_specs=P(("groups", "blk", "tile"), "sub"),
        check_vma=False,
    )
```
